32 devices in a mesh: dp: 8 (over z, x), feat: 4 (over y, core).
Axes of the slice: x: 2, y: 2, z: 4, core: 2. Of those that a mesh axis runs over, the one named last changes fastest.
Arguments:
- activations: bfloat16 [2048, 8192], P('dp', 'feat'), may hold values from -6 to 6
- cotangent: bfloat16 [2048, 1024], P('dp'), may hold values from -0.13183594 to 0.13183594
- weight: float32 [8192, 1024], P('feat'), may hold values from -0.0625 to 0.0625
- stats_old: float32 [4, 8, 4, 256, 256], P('feat', 'dp'), as said below
- owners: int32 [32, 4], replicated, may hold values from 0 to 7, as said below
- next_acts: bfloat16 [2048, 8192], P('dp', 'feat'), may hold values from -6 to 6
Outputs:
- weight_new: float32 [8192, 1024], P('feat')
- stats_new: float32 [4, 8, 4, 256, 256], P('feat', 'dp')
- next_out: bfloat16 [2048, 1024], P('dp', 'feat')
The draws below stay inside these ranges and needn't reach their ends.
Inputs may be any that keep to these rules, and one draw needn't show every extreme that they name: `owners`: blocks are grouped by the index of feat that holds their rows (8192 / (256 * 4) row blocks a group); in every group each dp index owns at most 4 blocks, and some dp index owns exactly 4. `stats_old`: every slot holds a symmetric positive definite matrix; slots that no block maps to are not read.
All inputs are finite; a program needn't handle non-finite values.
Results may differ from the reference program's by a relative error of at most 0.02.
Values may be sent and summed in bfloat16 or wider, within the bound.
A program may use at most 128 MiB of HBM per device.

```python
import jax
import jax.numpy as jnp
from jax import lax

D = 8192
COLS = 1024
BLOCK = 256
ITERS = 6
TOKENS = 2048
MOST = 4
N_DP = 8
N_FEAT = 4


def draw_owners(key, part):
    block_count = D // (BLOCK * N_FEAT) * (COLS // BLOCK)
    group_keys = jax.random.split(jax.random.fold_in(key, 11), N_FEAT)
    order_keys = jax.random.split(jax.random.fold_in(key, 23), N_FEAT)
    chosen = jax.vmap(lambda sub: jax.random.permutation(sub, N_DP))(group_keys).astype(jnp.int32)
    place_ids = jnp.arange(block_count, dtype=jnp.int32)
    pick_ids = jnp.where(place_ids < MOST, 0, 1 + jnp.maximum(place_ids - MOST, 0) % (N_DP - 1)).astype(jnp.int32)
    listing = chosen[:, pick_ids]
    shuffle = jax.vmap(lambda sub: jax.random.permutation(sub, block_count))(order_keys).astype(jnp.int32)
    placed = jnp.take_along_axis(listing, shuffle, axis=1)
    return placed.reshape(D // BLOCK, COLS // BLOCK).astype(jnp.int32)


def draw_stats_old(key, part):
    shape = (N_FEAT, N_DP, MOST, BLOCK, BLOCK)
    base = jax.random.normal(jax.random.fold_in(key, 31), shape, jnp.float32)
    product = jnp.einsum('abcij,abckj->abcik', base, base, precision=lax.Precision.HIGHEST) / BLOCK
    identity = jnp.eye(BLOCK, dtype=jnp.float32)
    return (product + 0.125 * identity).astype(jnp.float32)


def block_scale(key, dims, shards, smallest, high):
    factor_of = 1.0
    for dim, blocks in shards:
        draws = jax.random.uniform(jax.random.fold_in(jax.random.fold_in(key, 6), dim), (blocks,), jnp.float32, smallest / len(shards), high / len(shards))
        factor_of = factor_of * jnp.repeat(jnp.exp(draws), dims[dim] // blocks).reshape((-1,) + (1,) * (len(dims) - 1 - dim))
    return factor_of


def noise(own_key, dims, spread, limit, cuts=(), kind=jnp.bfloat16):
    result = spread * jax.random.normal(own_key, dims, jnp.float32)
    if cuts:
        result = result * block_scale(own_key, dims, cuts, -0.22, 0.18)
    return jnp.clip(result, -limit, limit).astype(kind)


def setup_inputs(seed: int = 0) -> dict:
    key_list = jax.random.split(jax.random.key(seed), 7)
    return {
        "activations": noise(key_list[0], (TOKENS, D), 1.0, 6.0, ((0, 8), (1, 4))),
        "cotangent": noise(key_list[1], (TOKENS, COLS), (TOKENS ** -0.5), 0.13183594, ((0, 8),)),
        "weight": noise(key_list[2], (D, COLS), D ** -0.5, 0.0625, ((0, 4),), jnp.float32),
        "stats_old": draw_stats_old(jax.random.fold_in(key_list[6], 71), 0),
        "owners": draw_owners(jax.random.fold_in(key_list[6], 71), 0),
        "next_acts": noise(key_list[5], (TOKENS, D), 1.0, 6.0, ((0, 8), (1, 4))),
    }


decay_rate = 0.9
step_rate = 0.01

def newton_root(stats):
    width = stats.shape[0]
    identity = jnp.eye(width, dtype=jnp.float32)
    norm_value = jnp.sqrt(jnp.sum(stats * stats) + 1e-06)
    matrix = stats / norm_value
    iterate = identity
    for counter in range(ITERS):
        factor = (5.0 * identity - matrix) / 4.0
        factor_low = factor.astype(jnp.bfloat16)
        iterate = jnp.dot(iterate.astype(jnp.bfloat16), factor_low, preferred_element_type=jnp.float32)
        if counter + 1 < ITERS:
            square = jnp.dot(factor_low, factor_low, preferred_element_type=jnp.float32).astype(jnp.bfloat16)
            fourth = jnp.dot(square, square, preferred_element_type=jnp.float32).astype(jnp.bfloat16)
            matrix = jnp.dot(fourth, matrix.astype(jnp.bfloat16), preferred_element_type=jnp.float32)
    return iterate * norm_value ** (-0.25)

def one_block(pair):
    grad_block, old_stats = pair
    gram = jnp.dot(grad_block, grad_block.T, preferred_element_type=jnp.float32) / BLOCK
    renewed = decay_rate * old_stats + (1.0 - decay_rate) * gram
    root_matrix = newton_root(renewed)
    update = jnp.dot(root_matrix.astype(jnp.bfloat16), grad_block, preferred_element_type=jnp.float32)
    return (renewed, update)

def reference(activations, cotangent, weight, stats_old, owners, next_acts):
    grad = jnp.dot(activations.T, cotangent, preferred_element_type=jnp.float32)
    grad_low = grad.astype(jnp.bfloat16)
    row_count = D // BLOCK
    col_blocks = COLS // BLOCK
    block_count = D // (BLOCK * N_FEAT) * col_blocks
    blocks = grad_low.reshape(row_count, BLOCK, col_blocks, BLOCK).transpose(0, 2, 1, 3).reshape(row_count * col_blocks, BLOCK, BLOCK)
    own_list = owners.reshape(-1).astype(jnp.int32)
    block_ids = jnp.arange(row_count * col_blocks, dtype=jnp.int32)
    group_id = block_ids // block_count
    same_owner = (own_list[:, None] == own_list[None, :]) & (group_id[:, None] == group_id[None, :]) & (block_ids[None, :] < block_ids[:, None])
    slot_of = lax.optimization_barrier(jnp.sum(same_owner.astype(jnp.int32), axis=1)).astype(jnp.int32)
    old_stats = stats_old[group_id, own_list, slot_of]
    renewed_all, update_all = lax.map(one_block, (blocks, old_stats))
    update = update_all.reshape(row_count, col_blocks, BLOCK, BLOCK).transpose(0, 2, 1, 3).reshape(D, COLS)
    weight_new = weight - step_rate * update
    stats_new = jnp.zeros(stats_old.shape, jnp.float32).at[group_id, own_list, slot_of].set(renewed_all)
    next_out = jnp.dot(next_acts, weight_new.astype(jnp.bfloat16), preferred_element_type=jnp.float32).astype(jnp.bfloat16)
    return (weight_new, stats_new, next_out)
```

```python
import functools

import jax
import jax.numpy as jnp
from jax import lax
from jax.experimental import pallas as pl
from jax.experimental.pallas import tpu as pltpu
from jax.sharding import PartitionSpec as P

ITERS = 6

decay_rate = 0.9
step_rate = 0.01
VMEM_BYTES = 48 * 1024 * 1024
REFRESH_BYTES = 20 * 1024 * 1024
APPLY_BYTES = 36 * 1024 * 1024
TOTAL_BYTES = 4 * 1024 * 1024


def spot(index, count):
    if count % 2:
        return index
    odd = lax.rem(index, 2)
    half = index // 2
    return (1 - odd) * half + odd * (count - 1 - half)


def at_spot(place, count):
    place = lax.rem(place + 2 * count, count)
    if count % 2:
        return place
    far = (2 * place) // count
    return (1 - far) * (2 * place) + far * (2 * (count - place) - 1)


def refresh_kernel(
    n, slots, width, row_ref, col_ref, act_ref, cot_ref, old_hbm, stats_ref, gath_ref,
    act_cut, cot_cut, old_ref, first_ref, acc_ref, grad_ref, mat_ref, iter_ref,
    rs_send, rs_recv, ag_send, ag_recv, act_sem, cot_sem, old_sem,
):
    me = lax.axis_index("dp")
    here = spot(me, n)
    after, before = at_spot(here + 1, n), at_spot(here - 1, n)
    forward = (slots + 1) // 2
    sign = [1 if k < forward else -1 for k in range(slots)]
    turns = sorted(range(slots), key=lambda k: (k % forward, k))
    target = {1: after, -1: before}

    barrier = pltpu.get_barrier_semaphore()
    for peer in (before, after):
        pl.semaphore_signal(
            barrier, inc=1, device_id={"dp": peer}, device_id_type=pl.DeviceIdType.MESH
        )

    cuts = [
        pltpu.make_async_copy(
            cot_ref.at[:, c * width : (c + 1) * width], cot_cut.at[c], cot_sem.at[c]
        )
        for c in range(cot_cut.shape[0])
    ] + [
        pltpu.make_async_copy(
            act_ref.at[:, r * width : (r + 1) * width], act_cut.at[r], act_sem.at[r]
        )
        for r in range(act_cut.shape[0])
    ]
    load_old = pltpu.make_async_copy(old_hbm, old_ref, old_sem)
    for cut in cuts:
        cut.start()
    load_old.start()

    def term(place, k):
        index = at_spot(place, n) * slots + k
        return lax.dot_general(
            act_cut[row_ref[index]],
            cot_cut[col_ref[index]],
            (((0,), (0,)), ((), ())),
            preferred_element_type=jnp.float32,
        )

    def sum_copy(k, step, first=False):
        return pltpu.make_async_remote_copy(
            src_ref=first_ref.at[k] if first else acc_ref.at[k, step - 1],
            dst_ref=acc_ref.at[k, step],
            send_sem=rs_send.at[k, step],
            recv_sem=rs_recv.at[k, step],
            device_id={"dp": target[sign[k]]},
            device_id_type=pl.DeviceIdType.MESH,
        )

    def gather_copy(k, step, owner):
        return pltpu.make_async_remote_copy(
            src_ref=gath_ref.at[owner, k],
            dst_ref=gath_ref.at[owner, k],
            send_sem=ag_send.at[k, step],
            recv_sem=ag_recv.at[k, step],
            device_id={"dp": target[sign[k]]},
            device_id_type=pl.DeviceIdType.MESH,
        )

    for cut in cuts:
        cut.wait()
    for k in turns:
        first_ref[k] = term(here - sign[k], k).astype(jnp.bfloat16)
    pl.semaphore_wait(barrier, 2)
    for k in turns:
        sum_copy(k, 0, True).start()

    def pass_on(step, _):
        for k in turns:
            own = term(here - sign[k] * (2 + step), k)
            sum_copy(k, step, True).wait_recv()
            acc_ref[k, step] = (acc_ref[k, step].astype(jnp.float32) + own).astype(jnp.bfloat16)
            sum_copy(k, step + 1).start()
        return 0

    lax.fori_loop(0, n - 2, pass_on, 0)
    for k in turns:
        own = term(here, k)
        sum_copy(k, n - 2, True).wait_recv()
        grad_ref[k] = (acc_ref[k, n - 2].astype(jnp.float32) + own).astype(jnp.bfloat16)

    load_old.wait()
    row = lax.broadcasted_iota(jnp.int32, (width, width), 0)
    col = lax.broadcasted_iota(jnp.int32, (width, width), 1)
    identity = jnp.where(row == col, 1.0, 0.0).astype(jnp.float32)
    dot = functools.partial(jnp.dot, preferred_element_type=jnp.float32)
    norms = []
    for k in range(slots):
        g = grad_ref[k]
        gram = (
            lax.dot_general(g, g, (((1,), (1,)), ((), ())), preferred_element_type=jnp.float32)
            / width
        )
        renewed = decay_rate * old_ref[k] + (1.0 - decay_rate) * gram
        stats_ref[k] = renewed
        norm = jnp.sqrt(jnp.sum(renewed * renewed, keepdims=True) + 1e-06)
        norms.append(norm)
        mat_ref[k] = renewed / norm

    def factors():
        return [((5.0 * identity - mat_ref[k]) / 4.0).astype(jnp.bfloat16) for k in range(slots)]

    def advance(low):
        square = [dot(low[k], low[k]).astype(jnp.bfloat16) for k in range(slots)]
        fourth = [dot(square[k], square[k]).astype(jnp.bfloat16) for k in range(slots)]
        for k in range(slots):
            mat_ref[k] = dot(fourth[k], mat_ref[k].astype(jnp.bfloat16))

    low = factors()
    for k in range(slots):
        iter_ref[k] = low[k]
    advance(low)

    def newton_step(step, _):
        low = factors()
        for k in range(slots):
            iter_ref[k] = dot(iter_ref[k], low[k]).astype(jnp.bfloat16)
        advance(low)
        return 0

    lax.fori_loop(1, ITERS - 1, newton_step, 0)
    low = factors()
    for k in turns:
        root = dot(iter_ref[k], low[k]) * norms[k] ** (-0.25)
        gath_ref[me, k] = dot(root.astype(jnp.bfloat16), grad_ref[k]).astype(jnp.bfloat16)
        gather_copy(k, 0, me).start()

    def relay(step, _):
        for k in turns:
            owner = at_spot(here - sign[k] * (1 + step), n)
            gather_copy(k, step, owner).wait_recv()
            gather_copy(k, step + 1, owner).start()
        return 0

    lax.fori_loop(0, n - 2, relay, 0)
    for k in turns:
        owner = at_spot(here - sign[k] * (n - 1), n)
        gather_copy(k, n - 2, owner).wait_recv()

    def finish(step, _):
        for k in turns:
            sum_copy(k, step, True).wait_send()
            gather_copy(k, step, me).wait_send()
        return 0

    lax.fori_loop(0, n - 1, finish, 0)


def refresh(n, row_of, col_of, activations, cotangent, old):
    slots, width, _ = old.shape
    tokens = activations.shape[0]
    vmem = pl.BlockSpec(memory_space=pltpu.VMEM)
    smem = pl.BlockSpec(memory_space=pltpu.SMEM)
    hbm = pl.BlockSpec(memory_space=pltpu.HBM)
    dma = pltpu.SemaphoreType.DMA
    low = jnp.bfloat16
    return pl.pallas_call(
        functools.partial(refresh_kernel, n, slots, width),
        out_shape=(
            jax.ShapeDtypeStruct((slots, width, width), jnp.float32),
            jax.ShapeDtypeStruct((n, slots, width, width), low),
        ),
        in_specs=[smem, smem, hbm, hbm, hbm],
        out_specs=(vmem, vmem),
        scratch_shapes=[
            pltpu.VMEM((activations.shape[1] // width, tokens, width), low),
            pltpu.VMEM((cotangent.shape[1] // width, tokens, width), low),
            pltpu.VMEM((slots, width, width), jnp.float32),
            pltpu.VMEM((slots, width, width), low),
            pltpu.VMEM((slots, n - 1, width, width), low),
            pltpu.VMEM((slots, width, width), low),
            pltpu.VMEM((slots, width, width), jnp.float32),
            pltpu.VMEM((slots, width, width), low),
            dma((slots, n - 1)),
            dma((slots, n - 1)),
            dma((slots, n - 1)),
            dma((slots, n - 1)),
            dma((activations.shape[1] // width,)),
            dma((cotangent.shape[1] // width,)),
            dma,
        ],
        compiler_params=pltpu.CompilerParams(
            vmem_limit_bytes=REFRESH_BYTES if n * slots <= 32 else VMEM_BYTES,
            collective_id=0,
            has_side_effects=True,
        ),
        cost_estimate=pl.CostEstimate(
            flops=2 * slots * 31 * width**3, bytes_accessed=100_000_000, transcendentals=0
        ),
        name="refresh",
    )(row_of, col_of, *(pltpu.with_memory_space_constraint(x, pltpu.HBM) for x in (activations, cotangent, old)))


def total_kernel(n, part_ref, out_ref, near_ref, pair_ref, far_ref, near_send, near_recv, far_send, far_recv):
    me = lax.axis_index("feat")
    core = lax.rem(me, 2)
    here = me // 2
    chips = n // 2
    partner = here * 2 + 1 - core
    barrier = pltpu.get_barrier_semaphore()
    peers = [lax.rem(here + d, chips) * 2 + core for d in range(1, chips)]
    for peer in peers + [partner]:
        pl.semaphore_signal(
            barrier, inc=1, device_id={"feat": peer}, device_id_type=pl.DeviceIdType.MESH
        )
    pl.semaphore_wait(barrier, chips)

    def near_copy(d):
        place = lax.rem(here + d, chips) * 2 + 1 - core
        return pltpu.make_async_remote_copy(
            src_ref=part_ref.at[place],
            dst_ref=near_ref.at[d],
            send_sem=near_send.at[d],
            recv_sem=near_recv.at[d],
            device_id={"feat": partner},
            device_id_type=pl.DeviceIdType.MESH,
        )

    def far_copy(d):
        return pltpu.make_async_remote_copy(
            src_ref=pair_ref.at[d - 1],
            dst_ref=far_ref.at[d - 1],
            send_sem=far_send.at[d - 1],
            recv_sem=far_recv.at[d - 1],
            device_id={"feat": peers[d - 1]},
            device_id_type=pl.DeviceIdType.MESH,
        )

    def pair_sum(d):
        place = lax.rem(here + d, chips) * 2 + core
        own = part_ref[place].astype(jnp.float32)
        return own + near_ref[d].astype(jnp.float32)

    turns = list(range(1, chips)) + [0]
    for d in turns:
        near_copy(d).start()
    for d in turns[:-1]:
        near_copy(d).wait_recv()
        pair_ref[d - 1] = pair_sum(d).astype(pair_ref.dtype)
        far_copy(d).start()
    near_copy(0).wait_recv()
    total = pair_sum(0)
    for d in turns[:-1]:
        far_copy(d).wait_recv()
        total = total + far_ref[d - 1].astype(jnp.float32)
    out_ref[...] = total.astype(out_ref.dtype)
    for d in turns:
        near_copy(d).wait_send()
    for d in turns[:-1]:
        far_copy(d).wait_send()


def total_over_feat(n, parts):
    _, tokens, cols = parts.shape
    vmem = pl.BlockSpec(memory_space=pltpu.VMEM)
    dma = pltpu.SemaphoreType.DMA
    chips = n // 2
    return pl.pallas_call(
        functools.partial(total_kernel, n),
        out_shape=jax.ShapeDtypeStruct((tokens, cols), parts.dtype),
        in_specs=[vmem],
        out_specs=vmem,
        scratch_shapes=[
            pltpu.VMEM((chips, tokens, cols), parts.dtype),
            pltpu.VMEM((chips - 1, tokens, cols), parts.dtype),
            pltpu.VMEM((chips - 1, tokens, cols), parts.dtype),
            dma((chips,)),
            dma((chips,)),
            dma((chips - 1,)),
            dma((chips - 1,)),
        ],
        compiler_params=pltpu.CompilerParams(
            vmem_limit_bytes=TOTAL_BYTES, collective_id=1, has_side_effects=True
        ),
        name="total_over_feat",
    )(parts)


def apply_kernel(
    width, col_blocks, splits, place_ref, weight_ref, acts_ref, gath_ref, stats_ref,
    new_hbm, part_ref, stats_hbm, fresh_ref, low_ref, new_sem, stats_sem,
):
    row_blocks = weight_ref.shape[0] // width
    share = weight_ref.shape[1] // splits
    keep = pltpu.make_async_copy(stats_ref, stats_hbm, stats_sem)
    keep.start()
    writes = []
    for c in range(col_blocks):
        cols = slice(c * width, (c + 1) * width)
        for r in range(row_blocks):
            rows = slice(r * width, (r + 1) * width)
            update = gath_ref[place_ref[r * col_blocks + c]]
            fresh = weight_ref[rows, cols] - step_rate * update.astype(jnp.float32)
            fresh_ref[rows, cols] = fresh
            low_ref[c, rows, :] = fresh.astype(jnp.bfloat16)
        write = pltpu.make_async_copy(
            fresh_ref.at[:, cols], new_hbm.at[:, cols], new_sem.at[c]
        )
        write.start()
        writes.append(write)
        part = jnp.dot(acts_ref[...], low_ref[c], preferred_element_type=jnp.float32)
        part = part.astype(part_ref.dtype)
        if share >= width:
            spot_in = (c * width) % share
            part_ref[(c * width) // share, :, spot_in : spot_in + width] = part
        else:
            for f in range(width // share):
                part_ref[(c * width) // share + f] = part[:, f * share : (f + 1) * share]
    for write in writes:
        write.wait()
    keep.wait()


def apply_update(place, weight, acts, gathered, stats, splits):
    width = gathered.shape[-1]
    rows, cols = weight.shape
    tokens = acts.shape[0]
    share = cols // splits
    vmem = pl.BlockSpec(memory_space=pltpu.VMEM)
    hbm = pl.BlockSpec(memory_space=pltpu.HBM)
    return pl.pallas_call(
        functools.partial(apply_kernel, width, cols // width, splits),
        out_shape=(
            jax.ShapeDtypeStruct((rows, cols), jnp.float32),
            jax.ShapeDtypeStruct((splits, tokens, share), jnp.bfloat16),
            jax.ShapeDtypeStruct(stats.shape, stats.dtype),
        ),
        in_specs=[pl.BlockSpec(memory_space=pltpu.SMEM), vmem, vmem, vmem, vmem],
        out_specs=(hbm, vmem, hbm),
        scratch_shapes=[
            pltpu.VMEM((rows, cols), jnp.float32),
            pltpu.VMEM((cols // width, rows, width), jnp.bfloat16),
            pltpu.SemaphoreType.DMA((cols // width,)),
            pltpu.SemaphoreType.DMA,
        ],
        compiler_params=pltpu.CompilerParams(vmem_limit_bytes=APPLY_BYTES if gathered.size <= 1 << 21 else VMEM_BYTES),
        cost_estimate=pl.CostEstimate(
            flops=2 * rows * cols * tokens,
            bytes_accessed=8 * rows * cols + 2 * gathered.size,
            transcendentals=0,
        ),
        name="apply_update",
    )(place, weight, acts, gathered, stats)


def body(n_dp, n_feat, activations, cotangent, weight, stats_old, owners, next_acts):
    width = stats_old.shape[-1]
    slots = stats_old.shape[2]
    rows_dev, columns = weight.shape
    row_blocks = rows_dev // width
    col_blocks = columns // width
    block_count = row_blocks * col_blocks
    feat_index = lax.axis_index("feat")
    data_index = lax.axis_index("dp")
    own_list = lax.dynamic_slice_in_dim(owners, feat_index * row_blocks, row_blocks, 0).reshape(
        block_count
    )
    ids = jnp.arange(block_count, dtype=jnp.int32)
    slot_of = jnp.sum(
        ((own_list[:, None] == own_list[None, :]) & (ids[None, :] < ids[:, None])).astype(jnp.int32),
        axis=1,
    )
    place = own_list * slots + slot_of
    held = place[None, :] == jnp.arange(n_dp * slots, dtype=jnp.int32)[:, None]
    order = jnp.sum(jnp.where(held, ids[None, :], 0), axis=1)
    stats, gathered = refresh(
        n_dp, order // col_blocks, order % col_blocks, activations, cotangent, stats_old[0, 0]
    )
    if n_dp * slots != block_count:
        mine = (own_list == data_index)[None, :] & (slot_of[None, :] == jnp.arange(slots)[:, None])
        stats = jnp.where(jnp.any(mine, axis=1)[:, None, None], stats, 0.0)
    gathered = gathered.reshape(n_dp * slots, width, width)
    direct = columns % (128 * n_feat) == 0 and n_feat % 2 == 0 and n_feat > 2
    weight_new, parts, stats = apply_update(
        place, weight, next_acts, gathered, stats, n_feat if direct else 1
    )
    if direct:
        next_out = total_over_feat(n_feat, parts)
    else:
        next_out = lax.psum_scatter(parts[0], "feat", scatter_dimension=1, tiled=True)
    return (weight_new, stats[None, None], next_out)


def solution(mesh):
    placed = (
        P("dp", "feat"),
        P("dp", None),
        P("feat", None),
        P("feat", "dp", None, None, None),
        P(),
        P("dp", "feat"),
    )
    return jax.shard_map(
        functools.partial(body, mesh.shape["dp"], mesh.shape["feat"]),
        mesh=mesh,
        in_specs=placed,
        out_specs=(P("feat", None), P("feat", "dp", None, None, None), P("dp", "feat")),
        check_vma=False,
    )
```

```python
import functools

import jax
import jax.numpy as jnp
from jax import lax
from jax.experimental import pallas as pl
from jax.experimental.pallas import tpu as pltpu
from jax.sharding import PartitionSpec as P

ITERS = 6

decay_rate = 0.9
step_rate = 0.01
PIECES = 1
LAG = 0
HEAD = 15
VMEM_BYTES = 48 * 1024 * 1024
REFRESH_BYTES = 20 * 1024 * 1024
APPLY_BYTES = 36 * 1024 * 1024
TOTAL_BYTES = 4 * 1024 * 1024


def spot(index, count):
    if count % 2:
        return index
    odd = lax.rem(index, 2)
    half = index // 2
    return (1 - odd) * half + odd * (count - 1 - half)


def at_spot(place, count):
    place = lax.rem(place + 2 * count, count)
    if count % 2:
        return place
    far = (2 * place) // count
    return (1 - far) * (2 * place) + far * (2 * (count - place) - 1)


def refresh_kernel(
    n, slots, width, pieces, lag, row_ref, col_ref, act_ref, cot_ref, old_hbm, weight_hbm, next_hbm,
    stats_ref, gath_ref, weight_ref, next_ref,
    act_cut, cot_cut, old_ref, first_ref, acc_ref, grad_ref, mat_ref, iter_ref,
    rs_send, rs_recv, ag_send, ag_recv, act_sem, cot_sem, old_sem, ahead_sem,
):
    me = lax.axis_index("dp")
    here = spot(me, n)
    after, before = at_spot(here + 1, n), at_spot(here - 1, n)
    forward = (slots + 1) // 2
    sign = [1 if k < forward else -1 for k in range(slots)]
    early = [k for k in range(slots) if k % forward < (forward + 1) // 2]
    late = [k for k in range(slots) if k not in early]
    target = {1: after, -1: before}
    height = width // pieces
    cuts_of = [slice(q * height, (q + 1) * height) for q in range(pieces)]

    barrier = pltpu.get_barrier_semaphore()
    for peer in (before, after):
        pl.semaphore_signal(
            barrier, inc=1, device_id={"dp": peer}, device_id_type=pl.DeviceIdType.MESH
        )

    cuts = [
        pltpu.make_async_copy(
            cot_ref.at[:, c * width : (c + 1) * width], cot_cut.at[c], cot_sem.at[c]
        )
        for c in range(cot_cut.shape[0])
    ] + [
        pltpu.make_async_copy(
            act_ref.at[:, r * width : (r + 1) * width], act_cut.at[r], act_sem.at[r]
        )
        for r in range(act_cut.shape[0])
    ]
    load_old = pltpu.make_async_copy(old_hbm, old_ref, old_sem)
    for cut in cuts:
        cut.start()
    load_old.start()

    def term(place, k):
        index = at_spot(place, n) * slots + k
        return lax.dot_general(
            act_cut[row_ref[index]],
            cot_cut[col_ref[index]],
            (((0,), (0,)), ((), ())),
            preferred_element_type=jnp.float32,
        )

    def sum_copy(k, step, q, first=False):
        rows = cuts_of[q]
        return pltpu.make_async_remote_copy(
            src_ref=first_ref.at[k, rows] if first else acc_ref.at[k, step - 1, rows],
            dst_ref=acc_ref.at[k, step, rows],
            send_sem=rs_send.at[k, step, q],
            recv_sem=rs_recv.at[k, step, q],
            device_id={"dp": target[sign[k]]},
            device_id_type=pl.DeviceIdType.MESH,
        )

    def gather_copy(k, step, q, owner):
        rows = cuts_of[q]
        return pltpu.make_async_remote_copy(
            src_ref=gath_ref.at[owner, k, rows],
            dst_ref=gath_ref.at[owner, k, rows],
            send_sem=ag_send.at[k, step, q],
            recv_sem=ag_recv.at[k, step, q],
            device_id={"dp": target[sign[k]]},
            device_id_type=pl.DeviceIdType.MESH,
        )

    def sum_first(k):
        for q in range(pieces):
            sum_copy(k, 0, q, True).start()

    def pass_on(k, step):
        own = term(here - sign[k] * (2 + step), k)
        for q in range(pieces):
            rows = cuts_of[q]
            sum_copy(k, step, q, True).wait_recv()
            total = acc_ref[k, step, rows].astype(jnp.float32) + own[rows]
            acc_ref[k, step, rows] = total.astype(jnp.bfloat16)
            sum_copy(k, step + 1, q).start()

    def settle(k):
        own = term(here, k)
        for q in range(pieces):
            rows = cuts_of[q]
            sum_copy(k, n - 2, q, True).wait_recv()
            total = acc_ref[k, n - 2, rows].astype(jnp.float32) + own[rows]
            grad_ref[k, rows] = total.astype(jnp.bfloat16)

    def relay(k, step):
        owner = at_spot(here - sign[k] * (1 + step), n)
        for q in range(pieces):
            gather_copy(k, step, q, owner).wait_recv()
            gather_copy(k, step + 1, q, owner).start()

    def arrive(k):
        owner = at_spot(here - sign[k] * (n - 1), n)
        for q in range(pieces):
            gather_copy(k, n - 2, q, owner).wait_recv()

    row = lax.broadcasted_iota(jnp.int32, (width, width), 0)
    col = lax.broadcasted_iota(jnp.int32, (width, width), 1)
    identity = jnp.where(row == col, 1.0, 0.0).astype(jnp.float32)
    dot = functools.partial(jnp.dot, preferred_element_type=jnp.float32)

    def newton(k):
        g = grad_ref[k]
        gram = lax.dot_general(g, g, (((1,), (1,)), ((), ())), preferred_element_type=jnp.float32)
        renewed = decay_rate * old_ref[k] + (1.0 - decay_rate) * (gram / width)
        stats_ref[k] = renewed
        norm = jnp.sqrt(jnp.sum(renewed * renewed, keepdims=True) + 1e-06)
        mat_ref[k] = renewed / norm
        yield
        for step in range(ITERS):
            low = ((5.0 * identity - mat_ref[k]) / 4.0).astype(jnp.bfloat16)
            if step == 0:
                iter_ref[k] = low
            elif step + 1 < ITERS:
                iter_ref[k] = dot(iter_ref[k], low).astype(jnp.bfloat16)
            if step + 1 < ITERS:
                square = dot(low, low).astype(jnp.bfloat16)
                yield
                fourth = dot(square, square).astype(jnp.bfloat16)
                yield
                mat_ref[k] = dot(fourth, mat_ref[k].astype(jnp.bfloat16))
                yield
        root = dot(iter_ref[k], low) * norm ** (-0.25)
        yield
        gath_ref[me, k] = dot(root.astype(jnp.bfloat16), grad_ref[k]).astype(jnp.bfloat16)
        for q in range(pieces):
            gather_copy(k, 0, q, me).start()

    def advance(works, count=None):
        while works and count != 0:
            works = [work for work in works if next(work, True) is None]
            count = None if count is None else count - 1
        return works

    def loop(start, stop, body):
        lax.fori_loop(start, stop, lambda i, _: (body(i), 0)[1], 0)

    for cut in cuts:
        cut.wait()
    for k in early:
        first_ref[k] = term(here - sign[k], k).astype(jnp.bfloat16)
    pl.semaphore_wait(barrier, 2)
    for k in early:
        sum_first(k)
    ahead = [
        pltpu.make_async_copy(weight_hbm, weight_ref, ahead_sem.at[0]),
        pltpu.make_async_copy(next_hbm, next_ref, ahead_sem.at[1]),
    ]
    for load in ahead:
        load.start()
    for k in late:
        first_ref[k] = term(here - sign[k], k).astype(jnp.bfloat16)

    def both(one, two, shift, step):
        for k in early:
            one(k, step)
        for k in late:
            two(k, step - shift)

    loop(0, lag, lambda i: [pass_on(k, i) for k in early])
    for k in late:
        sum_first(k)
    loop(lag, n - 2, functools.partial(both, pass_on, pass_on, lag))
    for k in early:
        settle(k)
    load_old.wait()
    works = advance([newton(k) for k in early], HEAD)
    for i in range(n - 2 - lag, n - 2):
        for k in late:
            pass_on(k, i)
    for k in late:
        settle(k)
    advance(works + [newton(k) for k in late])
    loop(0, n - 2, functools.partial(both, relay, relay, 0))
    for k in early:
        arrive(k)
    for k in late:
        arrive(k)

    for load in ahead:
        load.wait()

    def finish(step):
        for k in range(slots):
            for q in range(pieces):
                sum_copy(k, step, q, True).wait_send()
                gather_copy(k, step, q, me).wait_send()

    loop(0, n - 1, finish)


def refresh(n, row_of, col_of, activations, cotangent, old, weight, next_acts):
    slots, width, _ = old.shape
    pieces = PIECES if n * slots <= 32 else 1
    tokens = activations.shape[0]
    vmem = pl.BlockSpec(memory_space=pltpu.VMEM)
    smem = pl.BlockSpec(memory_space=pltpu.SMEM)
    hbm = pl.BlockSpec(memory_space=pltpu.HBM)
    dma = pltpu.SemaphoreType.DMA
    low = jnp.bfloat16
    return pl.pallas_call(
        functools.partial(refresh_kernel, n, slots, width, pieces, LAG),
        out_shape=(
            jax.ShapeDtypeStruct((slots, width, width), jnp.float32),
            jax.ShapeDtypeStruct((n, slots, width, width), low),
            jax.ShapeDtypeStruct(weight.shape, weight.dtype),
            jax.ShapeDtypeStruct(next_acts.shape, next_acts.dtype),
        ),
        in_specs=[smem, smem, hbm, hbm, hbm, hbm, hbm],
        out_specs=(vmem, vmem, vmem, vmem),
        scratch_shapes=[
            pltpu.VMEM((activations.shape[1] // width, tokens, width), low),
            pltpu.VMEM((cotangent.shape[1] // width, tokens, width), low),
            pltpu.VMEM((slots, width, width), jnp.float32),
            pltpu.VMEM((slots, width, width), low),
            pltpu.VMEM((slots, n - 1, width, width), low),
            pltpu.VMEM((slots, width, width), low),
            pltpu.VMEM((slots, width, width), jnp.float32),
            pltpu.VMEM((slots, width, width), low),
            dma((slots, n - 1, pieces)),
            dma((slots, n - 1, pieces)),
            dma((slots, n - 1, pieces)),
            dma((slots, n - 1, pieces)),
            dma((activations.shape[1] // width,)),
            dma((cotangent.shape[1] // width,)),
            dma,
            dma((2,)),
        ],
        compiler_params=pltpu.CompilerParams(
            vmem_limit_bytes=REFRESH_BYTES if n * slots <= 32 else VMEM_BYTES,
            collective_id=0,
            has_side_effects=True,
        ),
        cost_estimate=pl.CostEstimate(
            flops=2 * slots * 31 * width**3, bytes_accessed=100_000_000, transcendentals=0
        ),
        name="refresh",
    )(
        row_of, col_of,
        *(pltpu.with_memory_space_constraint(x, pltpu.HBM) for x in (activations, cotangent, old, weight, next_acts)),
    )


def total_kernel(n, part_ref, out_ref, near_ref, pair_ref, far_ref, near_send, near_recv, far_send, far_recv):
    me = lax.axis_index("feat")
    core = lax.rem(me, 2)
    here = me // 2
    chips = n // 2
    partner = here * 2 + 1 - core
    barrier = pltpu.get_barrier_semaphore()
    peers = [lax.rem(here + d, chips) * 2 + core for d in range(1, chips)]
    for peer in peers + [partner]:
        pl.semaphore_signal(
            barrier, inc=1, device_id={"feat": peer}, device_id_type=pl.DeviceIdType.MESH
        )
    pl.semaphore_wait(barrier, chips)

    def near_copy(d):
        place = lax.rem(here + d, chips) * 2 + 1 - core
        return pltpu.make_async_remote_copy(
            src_ref=part_ref.at[place],
            dst_ref=near_ref.at[d],
            send_sem=near_send.at[d],
            recv_sem=near_recv.at[d],
            device_id={"feat": partner},
            device_id_type=pl.DeviceIdType.MESH,
        )

    def far_copy(d):
        return pltpu.make_async_remote_copy(
            src_ref=pair_ref.at[d - 1],
            dst_ref=far_ref.at[d - 1],
            send_sem=far_send.at[d - 1],
            recv_sem=far_recv.at[d - 1],
            device_id={"feat": peers[d - 1]},
            device_id_type=pl.DeviceIdType.MESH,
        )

    def pair_sum(d):
        place = lax.rem(here + d, chips) * 2 + core
        own = part_ref[place].astype(jnp.float32)
        return own + near_ref[d].astype(jnp.float32)

    turns = list(range(1, chips)) + [0]
    for d in turns:
        near_copy(d).start()
    for d in turns[:-1]:
        near_copy(d).wait_recv()
        pair_ref[d - 1] = pair_sum(d).astype(pair_ref.dtype)
        far_copy(d).start()
    near_copy(0).wait_recv()
    total = pair_sum(0)
    for d in turns[:-1]:
        far_copy(d).wait_recv()
        total = total + far_ref[d - 1].astype(jnp.float32)
    out_ref[...] = total.astype(out_ref.dtype)
    for d in turns:
        near_copy(d).wait_send()
    for d in turns[:-1]:
        far_copy(d).wait_send()


def total_over_feat(n, parts):
    _, tokens, cols = parts.shape
    vmem = pl.BlockSpec(memory_space=pltpu.VMEM)
    dma = pltpu.SemaphoreType.DMA
    chips = n // 2
    return pl.pallas_call(
        functools.partial(total_kernel, n),
        out_shape=jax.ShapeDtypeStruct((tokens, cols), parts.dtype),
        in_specs=[vmem],
        out_specs=vmem,
        scratch_shapes=[
            pltpu.VMEM((chips, tokens, cols), parts.dtype),
            pltpu.VMEM((chips - 1, tokens, cols), parts.dtype),
            pltpu.VMEM((chips - 1, tokens, cols), parts.dtype),
            dma((chips,)),
            dma((chips,)),
            dma((chips - 1,)),
            dma((chips - 1,)),
        ],
        compiler_params=pltpu.CompilerParams(
            vmem_limit_bytes=TOTAL_BYTES, collective_id=1, has_side_effects=True
        ),
        name="total_over_feat",
    )(parts)


def apply_kernel(
    width, col_blocks, splits, place_ref, weight_ref, acts_ref, gath_ref, stats_ref,
    new_hbm, part_ref, stats_hbm, fresh_ref, low_ref, new_sem, stats_sem,
):
    row_blocks = weight_ref.shape[0] // width
    share = weight_ref.shape[1] // splits
    keep = pltpu.make_async_copy(stats_ref, stats_hbm, stats_sem)
    keep.start()
    writes = []

    def renew(c, r):
        rows, cols = slice(r * width, (r + 1) * width), slice(c * width, (c + 1) * width)
        update = gath_ref[place_ref[r * col_blocks + c]]
        fresh = weight_ref[rows, cols] - step_rate * update.astype(jnp.float32)
        fresh_ref[rows, cols] = fresh
        low_ref[c, rows, :] = fresh.astype(jnp.bfloat16)

    def write(c):
        cols = slice(c * width, (c + 1) * width)
        copy = pltpu.make_async_copy(fresh_ref.at[:, cols], new_hbm.at[:, cols], new_sem.at[c])
        copy.start()
        writes.append(copy)

    for r in range(row_blocks):
        renew(0, r)
    write(0)
    for c in range(col_blocks):
        part = jnp.zeros((acts_ref.shape[0], width), jnp.float32)
        for r in range(row_blocks):
            rows = slice(r * width, (r + 1) * width)
            part = part + jnp.dot(
                acts_ref[:, rows], low_ref[c, rows, :], preferred_element_type=jnp.float32
            )
            if c + 1 < col_blocks:
                renew(c + 1, r)
        if c + 1 < col_blocks:
            write(c + 1)
        part = part.astype(part_ref.dtype)
        if share >= width:
            spot_in = (c * width) % share
            part_ref[(c * width) // share, :, spot_in : spot_in + width] = part
        else:
            for f in range(width // share):
                part_ref[(c * width) // share + f] = part[:, f * share : (f + 1) * share]
    for copy in writes:
        copy.wait()
    keep.wait()


def apply_update(place, weight, acts, gathered, stats, splits):
    width = gathered.shape[-1]
    rows, cols = weight.shape
    tokens = acts.shape[0]
    share = cols // splits
    vmem = pl.BlockSpec(memory_space=pltpu.VMEM)
    hbm = pl.BlockSpec(memory_space=pltpu.HBM)
    return pl.pallas_call(
        functools.partial(apply_kernel, width, cols // width, splits),
        out_shape=(
            jax.ShapeDtypeStruct((rows, cols), jnp.float32),
            jax.ShapeDtypeStruct((splits, tokens, share), jnp.bfloat16),
            jax.ShapeDtypeStruct(stats.shape, stats.dtype),
        ),
        in_specs=[pl.BlockSpec(memory_space=pltpu.SMEM), vmem, vmem, vmem, vmem],
        out_specs=(hbm, vmem, hbm),
        scratch_shapes=[
            pltpu.VMEM((rows, cols), jnp.float32),
            pltpu.VMEM((cols // width, rows, width), jnp.bfloat16),
            pltpu.SemaphoreType.DMA((cols // width,)),
            pltpu.SemaphoreType.DMA,
        ],
        compiler_params=pltpu.CompilerParams(
            vmem_limit_bytes=APPLY_BYTES if gathered.size <= 1 << 21 else VMEM_BYTES,
        ),
        cost_estimate=pl.CostEstimate(
            flops=2 * rows * cols * tokens,
            bytes_accessed=8 * rows * cols + 2 * gathered.size,
            transcendentals=0,
        ),
        name="apply_update",
    )(place, weight, acts, gathered, stats)


def body(n_dp, n_feat, activations, cotangent, weight, stats_old, owners, next_acts):
    width = stats_old.shape[-1]
    slots = stats_old.shape[2]
    rows_dev, columns = weight.shape
    row_blocks = rows_dev // width
    col_blocks = columns // width
    block_count = row_blocks * col_blocks
    feat_index = lax.axis_index("feat")
    data_index = lax.axis_index("dp")
    own_list = lax.dynamic_slice_in_dim(owners, feat_index * row_blocks, row_blocks, 0).reshape(
        block_count
    )
    ids = jnp.arange(block_count, dtype=jnp.int32)
    slot_of = jnp.sum(
        ((own_list[:, None] == own_list[None, :]) & (ids[None, :] < ids[:, None])).astype(jnp.int32),
        axis=1,
    )
    place = own_list * slots + slot_of
    held = place[None, :] == jnp.arange(n_dp * slots, dtype=jnp.int32)[:, None]
    order = jnp.sum(jnp.where(held, ids[None, :], 0), axis=1)
    stats, gathered, weight, next_acts = refresh(
        n_dp, order // col_blocks, order % col_blocks, activations, cotangent, stats_old[0, 0],
        weight, next_acts,
    )
    if n_dp * slots != block_count:
        mine = (own_list == data_index)[None, :] & (slot_of[None, :] == jnp.arange(slots)[:, None])
        stats = jnp.where(jnp.any(mine, axis=1)[:, None, None], stats, 0.0)
    gathered = gathered.reshape(n_dp * slots, width, width)
    direct = columns % (128 * n_feat) == 0 and n_feat % 2 == 0 and n_feat > 2
    weight_new, parts, stats = apply_update(
        place, weight, next_acts, gathered, stats, n_feat if direct else 1
    )
    if direct:
        next_out = total_over_feat(n_feat, parts)
    else:
        next_out = lax.psum_scatter(parts[0], "feat", scatter_dimension=1, tiled=True)
    return (weight_new, stats[None, None], next_out)


def solution(mesh):
    placed = (
        P("dp", "feat"),
        P("dp", None),
        P("feat", None),
        P("feat", "dp", None, None, None),
        P(),
        P("dp", "feat"),
    )
    return jax.shard_map(
        functools.partial(body, mesh.shape["dp"], mesh.shape["feat"]),
        mesh=mesh,
        in_specs=placed,
        out_specs=(P("feat", None), P("feat", "dp", None, None, None), P("dp", "feat")),
        check_vma=False,
    )
```

```python
import functools

import jax
import jax.numpy as jnp
from jax import lax
from jax.experimental import pallas as pl
from jax.experimental.pallas import tpu as pltpu
from jax.sharding import PartitionSpec as P

ITERS = 6

decay_rate = 0.9
step_rate = 0.01
HEAD = 18
TAIL = 0
VMEM_BYTES = 48 * 1024 * 1024
REFRESH_BYTES = 20 * 1024 * 1024
APPLY_BYTES = 36 * 1024 * 1024
TOTAL_BYTES = 4 * 1024 * 1024


def spot(index, count):
    if count % 2:
        return index
    odd = lax.rem(index, 2)
    half = index // 2
    return (1 - odd) * half + odd * (count - 1 - half)


def at_spot(place, count):
    place = lax.rem(place + 2 * count, count)
    if count % 2:
        return place
    far = (2 * place) // count
    return (1 - far) * (2 * place) + far * (2 * (count - place) - 1)


def refresh_kernel(
    n, slots, width, row_ref, col_ref, act_ref, cot_ref, old_hbm, weight_hbm, next_hbm,
    stats_ref, gath_ref, weight_ref, next_ref,
    act_cut, cot_cut, old_ref, first_ref, acc_ref, grad_ref, mat_ref, iter_ref,
    rs_send, rs_recv, ag_send, ag_recv, act_sem, cot_sem, old_sem, ahead_sem,
):
    me = lax.axis_index("dp")
    here = spot(me, n)
    after, before = at_spot(here + 1, n), at_spot(here - 1, n)
    early = list(range((slots + 1) // 2))
    late = list(range(len(early), slots))
    target = {1: after, -1: before}
    least = (n - 1) // 2
    sides = [(1, -1) if k % 2 == 0 else (-1, 1) for k in range(slots)]
    reach = [{one: n - 1 - least, two: least} for one, two in sides]
    far = [[s for s in sides[k] if reach[k][s] > least] for k in range(slots)]

    barrier = pltpu.get_barrier_semaphore()
    for peer in (before, after):
        pl.semaphore_signal(
            barrier, inc=1, device_id={"dp": peer}, device_id_type=pl.DeviceIdType.MESH
        )

    cuts = [
        pltpu.make_async_copy(
            cot_ref.at[:, c * width : (c + 1) * width], cot_cut.at[c], cot_sem.at[c]
        )
        for c in range(cot_cut.shape[0])
    ] + [
        pltpu.make_async_copy(
            act_ref.at[:, r * width : (r + 1) * width], act_cut.at[r], act_sem.at[r]
        )
        for r in range(act_cut.shape[0])
    ]
    load_old = pltpu.make_async_copy(old_hbm, old_ref, old_sem)
    for cut in cuts:
        cut.start()
    load_old.start()

    def term(place, k):
        index = at_spot(place, n) * slots + k
        return lax.dot_general(
            act_cut[row_ref[index]],
            cot_cut[col_ref[index]],
            (((0,), (0,)), ((), ())),
            preferred_element_type=jnp.float32,
        )

    def slot_copy(ref, sems, k, s, step, src):
        spot_of = (0 if s == 1 else reach[k][1]) + step
        return pltpu.make_async_remote_copy(
            src_ref=src,
            dst_ref=ref(spot_of),
            send_sem=sems[0].at[k, spot_of],
            recv_sem=sems[1].at[k, spot_of],
            device_id={"dp": target[s]},
            device_id_type=pl.DeviceIdType.MESH,
        )

    def sum_copy(k, s, step, first=False):
        before_it = (0 if s == 1 else reach[k][1]) + step - 1
        src = first_ref.at[k, (1 - s) // 2] if first else acc_ref.at[k, before_it]
        return slot_copy(lambda i: acc_ref.at[k, i], (rs_send, rs_recv), k, s, step, src)

    def gather_copy(k, s, step, owner):
        block = gath_ref.at[owner, k]
        return slot_copy(lambda i: block, (ag_send, ag_recv), k, s, step, block)

    def arrived(k, s, step):
        sum_copy(k, s, step, True).wait_recv()
        return acc_ref[k, (0 if s == 1 else reach[k][1]) + step].astype(jnp.float32)

    def sum_open(k, s):
        first_ref[k, (1 - s) // 2] = term(here + s * reach[k][s], k).astype(jnp.bfloat16)

    def pass_on(k, s, step):
        own = term(here + s * (reach[k][s] - step), k)
        total = (arrived(k, s, step - 1) + own).astype(jnp.bfloat16)
        acc_ref[k, (0 if s == 1 else reach[k][1]) + step - 1] = total
        sum_copy(k, s, step).start()

    def settle(k):
        total = term(here, k)
        for s in sides[k]:
            total = total + arrived(k, s, reach[k][s] - 1)
        grad_ref[k] = total.astype(jnp.bfloat16)

    def relay(k, s, step):
        owner = at_spot(here - s * (1 + step), n)
        gather_copy(k, s, step, owner).wait_recv()
        gather_copy(k, s, step + 1, owner).start()

    def arrive(k, s):
        last = reach[k][s] - 1
        gather_copy(k, s, last, at_spot(here - s * (1 + last), n)).wait_recv()

    row = lax.broadcasted_iota(jnp.int32, (width, width), 0)
    col = lax.broadcasted_iota(jnp.int32, (width, width), 1)
    identity = jnp.where(row == col, 1.0, 0.0).astype(jnp.float32)
    dot = functools.partial(jnp.dot, preferred_element_type=jnp.float32)

    def newton(k):
        g = grad_ref[k]
        gram = lax.dot_general(g, g, (((1,), (1,)), ((), ())), preferred_element_type=jnp.float32)
        renewed = decay_rate * old_ref[k] + (1.0 - decay_rate) * (gram / width)
        stats_ref[k] = renewed
        norm = jnp.sqrt(jnp.sum(renewed * renewed, keepdims=True) + 1e-06)
        mat_ref[k] = renewed / norm
        yield
        for step in range(ITERS):
            low = ((5.0 * identity - mat_ref[k]) / 4.0).astype(jnp.bfloat16)
            if step == 0:
                iter_ref[k] = low
            elif step + 1 < ITERS:
                iter_ref[k] = dot(iter_ref[k], low).astype(jnp.bfloat16)
            if step + 1 < ITERS:
                square = dot(low, low).astype(jnp.bfloat16)
                yield
                fourth = dot(square, square).astype(jnp.bfloat16)
                yield
                mat_ref[k] = dot(fourth, mat_ref[k].astype(jnp.bfloat16))
                yield
        root = dot(iter_ref[k], low) * norm ** (-0.25)
        yield
        gath_ref[me, k] = dot(root.astype(jnp.bfloat16), grad_ref[k]).astype(jnp.bfloat16)
        for s in sides[k]:
            gather_copy(k, s, 0, me).start()

    def advance(works, count=None):
        while works and count != 0:
            works = [work for work in works if next(work, True) is None]
            count = None if count is None else count - 1
        return works

    def loop(start, stop, body):
        lax.fori_loop(start, stop, lambda i, _: (body(i), 0)[1], 0)

    for cut in cuts:
        cut.wait()
    def arms(group, ends=sides):
        return [(k, s) for k in group for s in ends[k]]

    for k, s in arms(early):
        sum_open(k, s)
        if (k, s) == (early[0], sides[early[0]][0]):
            pl.semaphore_wait(barrier, 2)
        sum_copy(k, s, 0, True).start()
    ahead = [
        pltpu.make_async_copy(weight_hbm, weight_ref, ahead_sem.at[0]),
        pltpu.make_async_copy(next_hbm, next_ref, ahead_sem.at[1]),
    ]
    for load in ahead:
        load.start()
    for k, s in arms(late):
        sum_open(k, s)
    for k, s in arms(early):
        pass_on(k, s, 1)
    for k, s in arms(late):
        sum_copy(k, s, 0, True).start()

    def sum_step(i):
        for k, s in arms(early):
            pass_on(k, s, i)
        for k, s in arms(late):
            pass_on(k, s, i - 1)

    loop(2, least, sum_step)
    for k, s in arms(early, far):
        pass_on(k, s, least)
    for k, s in arms(late):
        pass_on(k, s, least - 1)
    for k in early:
        settle(k)
    load_old.wait()
    works = advance([newton(k) for k in early], HEAD)
    for k, s in arms(late, far):
        pass_on(k, s, least)
    advance(works)
    for k in late:
        settle(k)
    works = advance([newton(k) for k in late], TAIL)
    for k, s in arms(early):
        relay(k, s, 0)
    advance(works)

    def gather_step(i):
        for k, s in arms(early):
            relay(k, s, i)
        for k, s in arms(late):
            relay(k, s, i - 1)

    loop(1, least - 1, gather_step)
    for k, s in arms(early, far):
        relay(k, s, least - 1)
    for k, s in arms(late):
        relay(k, s, least - 2)
    for k, s in arms(late, far):
        relay(k, s, least - 1)
    for k, s in arms(early + late):
        arrive(k, s)
    for load in ahead:
        load.wait()

    for k, s in arms(early + late):
        for step in (0, reach[k][s]):
            if step:
                loop(1, step, lambda i, k=k, s=s: sum_copy(k, s, i).wait_send())
                loop(1, step, lambda i, k=k, s=s: gather_copy(k, s, i, me).wait_send())
            else:
                sum_copy(k, s, 0, True).wait_send()
                gather_copy(k, s, 0, me).wait_send()


def refresh(n, row_of, col_of, activations, cotangent, old, weight, next_acts):
    slots, width, _ = old.shape
    tokens = activations.shape[0]
    vmem = pl.BlockSpec(memory_space=pltpu.VMEM)
    smem = pl.BlockSpec(memory_space=pltpu.SMEM)
    hbm = pl.BlockSpec(memory_space=pltpu.HBM)
    dma = pltpu.SemaphoreType.DMA
    low = jnp.bfloat16
    return pl.pallas_call(
        functools.partial(refresh_kernel, n, slots, width),
        out_shape=(
            jax.ShapeDtypeStruct((slots, width, width), jnp.float32),
            jax.ShapeDtypeStruct((n, slots, width, width), low),
            jax.ShapeDtypeStruct(weight.shape, weight.dtype),
            jax.ShapeDtypeStruct(next_acts.shape, next_acts.dtype),
        ),
        in_specs=[smem, smem, hbm, hbm, hbm, hbm, hbm],
        out_specs=(vmem, vmem, vmem, vmem),
        scratch_shapes=[
            pltpu.VMEM((activations.shape[1] // width, tokens, width), low),
            pltpu.VMEM((cotangent.shape[1] // width, tokens, width), low),
            pltpu.VMEM((slots, width, width), jnp.float32),
            pltpu.VMEM((slots, 2, width, width), low),
            pltpu.VMEM((slots, n - 1, width, width), low),
            pltpu.VMEM((slots, width, width), low),
            pltpu.VMEM((slots, width, width), jnp.float32),
            pltpu.VMEM((slots, width, width), low),
            dma((slots, n - 1)),
            dma((slots, n - 1)),
            dma((slots, n - 1)),
            dma((slots, n - 1)),
            dma((activations.shape[1] // width,)),
            dma((cotangent.shape[1] // width,)),
            dma,
            dma((2,)),
        ],
        compiler_params=pltpu.CompilerParams(
            vmem_limit_bytes=REFRESH_BYTES if n * slots <= 32 else VMEM_BYTES,
            collective_id=0,
            has_side_effects=True,
        ),
        cost_estimate=pl.CostEstimate(
            flops=2 * slots * 31 * width**3, bytes_accessed=100_000_000, transcendentals=0
        ),
        name="refresh",
    )(
        row_of, col_of,
        *(pltpu.with_memory_space_constraint(x, pltpu.HBM) for x in (activations, cotangent, old, weight, next_acts)),
    )


def total_kernel(n, part_ref, out_ref, near_ref, pair_ref, far_ref, near_send, near_recv, far_send, far_recv):
    me = lax.axis_index("feat")
    core = lax.rem(me, 2)
    here = me // 2
    chips = n // 2
    partner = here * 2 + 1 - core
    barrier = pltpu.get_barrier_semaphore()
    peers = [lax.rem(here + d, chips) * 2 + core for d in range(1, chips)]
    for peer in peers + [partner]:
        pl.semaphore_signal(
            barrier, inc=1, device_id={"feat": peer}, device_id_type=pl.DeviceIdType.MESH
        )
    pl.semaphore_wait(barrier, chips)

    def near_copy(d):
        place = lax.rem(here + d, chips) * 2 + 1 - core
        return pltpu.make_async_remote_copy(
            src_ref=part_ref.at[place],
            dst_ref=near_ref.at[d],
            send_sem=near_send.at[d],
            recv_sem=near_recv.at[d],
            device_id={"feat": partner},
            device_id_type=pl.DeviceIdType.MESH,
        )

    def far_copy(d):
        return pltpu.make_async_remote_copy(
            src_ref=pair_ref.at[d - 1],
            dst_ref=far_ref.at[d - 1],
            send_sem=far_send.at[d - 1],
            recv_sem=far_recv.at[d - 1],
            device_id={"feat": peers[d - 1]},
            device_id_type=pl.DeviceIdType.MESH,
        )

    def pair_sum(d):
        place = lax.rem(here + d, chips) * 2 + core
        own = part_ref[place].astype(jnp.float32)
        return own + near_ref[d].astype(jnp.float32)

    turns = list(range(1, chips)) + [0]
    for d in turns:
        near_copy(d).start()
    for d in turns[:-1]:
        near_copy(d).wait_recv()
        pair_ref[d - 1] = pair_sum(d).astype(pair_ref.dtype)
        far_copy(d).start()
    near_copy(0).wait_recv()
    total = pair_sum(0)
    for d in turns[:-1]:
        far_copy(d).wait_recv()
        total = total + far_ref[d - 1].astype(jnp.float32)
    out_ref[...] = total.astype(out_ref.dtype)
    for d in turns:
        near_copy(d).wait_send()
    for d in turns[:-1]:
        far_copy(d).wait_send()


def total_over_feat(n, parts):
    _, tokens, cols = parts.shape
    vmem = pl.BlockSpec(memory_space=pltpu.VMEM)
    dma = pltpu.SemaphoreType.DMA
    chips = n // 2
    return pl.pallas_call(
        functools.partial(total_kernel, n),
        out_shape=jax.ShapeDtypeStruct((tokens, cols), parts.dtype),
        in_specs=[vmem],
        out_specs=vmem,
        scratch_shapes=[
            pltpu.VMEM((chips, tokens, cols), parts.dtype),
            pltpu.VMEM((chips - 1, tokens, cols), parts.dtype),
            pltpu.VMEM((chips - 1, tokens, cols), parts.dtype),
            dma((chips,)),
            dma((chips,)),
            dma((chips - 1,)),
            dma((chips - 1,)),
        ],
        compiler_params=pltpu.CompilerParams(
            vmem_limit_bytes=TOTAL_BYTES, collective_id=1, has_side_effects=True
        ),
        name="total_over_feat",
    )(parts)


def apply_kernel(
    width, col_blocks, splits, place_ref, weight_ref, acts_ref, gath_ref, stats_ref,
    new_hbm, part_ref, stats_hbm, fresh_ref, low_ref, new_sem, stats_sem,
):
    row_blocks = weight_ref.shape[0] // width
    share = weight_ref.shape[1] // splits
    keep = pltpu.make_async_copy(stats_ref, stats_hbm, stats_sem)
    keep.start()
    writes = []

    def renew(c, r):
        rows, cols = slice(r * width, (r + 1) * width), slice(c * width, (c + 1) * width)
        update = gath_ref[place_ref[r * col_blocks + c]]
        fresh = weight_ref[rows, cols] - step_rate * update.astype(jnp.float32)
        fresh_ref[rows, cols] = fresh
        low_ref[c, rows, :] = fresh.astype(jnp.bfloat16)
        copy = pltpu.make_async_copy(
            fresh_ref.at[rows, cols], new_hbm.at[rows, cols], new_sem.at[c, r]
        )
        copy.start()
        writes.append(copy)

    def write(c):
        return

        cols = slice(c * width, (c + 1) * width)
        copy = pltpu.make_async_copy(fresh_ref.at[:, cols], new_hbm.at[:, cols], new_sem.at[c])
        copy.start()
        writes.append(copy)

    for r in range(row_blocks):
        renew(0, r)
    write(0)
    for c in range(col_blocks):
        part = jnp.zeros((acts_ref.shape[0], width), jnp.float32)
        for r in range(row_blocks):
            rows = slice(r * width, (r + 1) * width)
            part = part + jnp.dot(
                acts_ref[:, rows], low_ref[c, rows, :], preferred_element_type=jnp.float32
            )
            if c + 1 < col_blocks:
                renew(c + 1, r)
        if c + 1 < col_blocks:
            write(c + 1)
        part = part.astype(part_ref.dtype)
        if share >= width:
            spot_in = (c * width) % share
            part_ref[(c * width) // share, :, spot_in : spot_in + width] = part
        else:
            for f in range(width // share):
                part_ref[(c * width) // share + f] = part[:, f * share : (f + 1) * share]
    for copy in writes:
        copy.wait()
    keep.wait()


def apply_update(place, weight, acts, gathered, stats, splits):
    width = gathered.shape[-1]
    rows, cols = weight.shape
    tokens = acts.shape[0]
    share = cols // splits
    vmem = pl.BlockSpec(memory_space=pltpu.VMEM)
    hbm = pl.BlockSpec(memory_space=pltpu.HBM)
    return pl.pallas_call(
        functools.partial(apply_kernel, width, cols // width, splits),
        out_shape=(
            jax.ShapeDtypeStruct((rows, cols), jnp.float32),
            jax.ShapeDtypeStruct((splits, tokens, share), jnp.bfloat16),
            jax.ShapeDtypeStruct(stats.shape, stats.dtype),
        ),
        in_specs=[pl.BlockSpec(memory_space=pltpu.SMEM), vmem, vmem, vmem, vmem],
        out_specs=(hbm, vmem, hbm),
        scratch_shapes=[
            pltpu.VMEM((rows, cols), jnp.float32),
            pltpu.VMEM((cols // width, rows, width), jnp.bfloat16),
            pltpu.SemaphoreType.DMA((cols // width, rows // width)),
            pltpu.SemaphoreType.DMA,
        ],
        compiler_params=pltpu.CompilerParams(
            vmem_limit_bytes=APPLY_BYTES if gathered.size <= 1 << 21 else VMEM_BYTES,
        ),
        cost_estimate=pl.CostEstimate(
            flops=2 * rows * cols * tokens,
            bytes_accessed=8 * rows * cols + 2 * gathered.size,
            transcendentals=0,
        ),
        name="apply_update",
    )(place, weight, acts, gathered, stats)


def body(n_dp, n_feat, activations, cotangent, weight, stats_old, owners, next_acts):
    width = stats_old.shape[-1]
    slots = stats_old.shape[2]
    rows_dev, columns = weight.shape
    row_blocks = rows_dev // width
    col_blocks = columns // width
    block_count = row_blocks * col_blocks
    feat_index = lax.axis_index("feat")
    data_index = lax.axis_index("dp")
    own_list = lax.dynamic_slice_in_dim(owners, feat_index * row_blocks, row_blocks, 0).reshape(
        block_count
    )
    ids = jnp.arange(block_count, dtype=jnp.int32)
    slot_of = jnp.sum(
        ((own_list[:, None] == own_list[None, :]) & (ids[None, :] < ids[:, None])).astype(jnp.int32),
        axis=1,
    )
    place = own_list * slots + slot_of
    held = place[None, :] == jnp.arange(n_dp * slots, dtype=jnp.int32)[:, None]
    order = jnp.sum(jnp.where(held, ids[None, :], 0), axis=1)
    stats, gathered, weight, next_acts = refresh(
        n_dp, order // col_blocks, order % col_blocks, activations, cotangent, stats_old[0, 0],
        weight, next_acts,
    )
    if n_dp * slots != block_count:
        mine = (own_list == data_index)[None, :] & (slot_of[None, :] == jnp.arange(slots)[:, None])
        stats = jnp.where(jnp.any(mine, axis=1)[:, None, None], stats, 0.0)
    gathered = gathered.reshape(n_dp * slots, width, width)
    direct = columns % (128 * n_feat) == 0 and n_feat % 2 == 0 and n_feat > 2
    weight_new, parts, stats = apply_update(
        place, weight, next_acts, gathered, stats, n_feat if direct else 1
    )
    if direct:
        next_out = total_over_feat(n_feat, parts)
    else:
        next_out = lax.psum_scatter(parts[0], "feat", scatter_dimension=1, tiled=True)
    return (weight_new, stats[None, None], next_out)


def solution(mesh):
    placed = (
        P("dp", "feat"),
        P("dp", None),
        P("feat", None),
        P("feat", "dp", None, None, None),
        P(),
        P("dp", "feat"),
    )
    return jax.shard_map(
        functools.partial(body, mesh.shape["dp"], mesh.shape["feat"]),
        mesh=mesh,
        in_specs=placed,
        out_specs=(P("feat", None), P("feat", "dp", None, None, None), P("dp", "feat")),
        check_vma=False,
    )
```

```python
import functools

import jax
import jax.numpy as jnp
from jax import lax
from jax.experimental import pallas as pl
from jax.experimental.pallas import tpu as pltpu
from jax.sharding import PartitionSpec as P

ITERS = 6

decay_rate = 0.9
step_rate = 0.01
HEAD = 18
TAIL = 4
VMEM_BYTES = 48 * 1024 * 1024
REFRESH_BYTES = 20 * 1024 * 1024
APPLY_BYTES = 36 * 1024 * 1024
TOTAL_BYTES = 4 * 1024 * 1024


def spot(index, count):
    if count % 2:
        return index
    odd = lax.rem(index, 2)
    half = index // 2
    return (1 - odd) * half + odd * (count - 1 - half)


def at_spot(place, count):
    place = lax.rem(place + 2 * count, count)
    if count % 2:
        return place
    far = (2 * place) // count
    return (1 - far) * (2 * place) + far * (2 * (count - place) - 1)


def refresh_kernel(
    n, slots, width, row_ref, col_ref, act_ref, cot_ref, old_hbm, weight_hbm, next_hbm,
    stats_ref, gath_ref, weight_ref, next_ref,
    act_cut, cot_cut, old_ref, first_ref, acc_ref, grad_ref, mat_ref, iter_ref,
    rs_send, rs_recv, ag_send, ag_recv, act_sem, cot_sem, old_sem, ahead_sem,
):
    me = lax.axis_index("dp")
    here = spot(me, n)
    after, before = at_spot(here + 1, n), at_spot(here - 1, n)
    early = list(range((slots + 1) // 2))
    late = list(range(len(early), slots))
    target = {1: after, -1: before}
    least = (n - 1) // 2
    sides = [(1, -1) if k % 2 == 0 else (-1, 1) for k in range(slots)]
    reach = [{one: n - 1 - least, two: least} for one, two in sides]
    far = [[s for s in sides[k] if reach[k][s] > least] for k in range(slots)]

    barrier = pltpu.get_barrier_semaphore()
    for peer in (before, after):
        pl.semaphore_signal(
            barrier, inc=1, device_id={"dp": peer}, device_id_type=pl.DeviceIdType.MESH
        )

    cuts = [
        pltpu.make_async_copy(
            cot_ref.at[:, c * width : (c + 1) * width], cot_cut.at[c], cot_sem.at[c]
        )
        for c in range(cot_cut.shape[0])
    ] + [
        pltpu.make_async_copy(
            act_ref.at[:, r * width : (r + 1) * width], act_cut.at[r], act_sem.at[r]
        )
        for r in range(act_cut.shape[0])
    ]
    load_old = pltpu.make_async_copy(old_hbm, old_ref, old_sem)
    for cut in cuts:
        cut.start()
    load_old.start()

    def term(place, k):
        index = at_spot(place, n) * slots + k
        return lax.dot_general(
            act_cut[row_ref[index]],
            cot_cut[col_ref[index]],
            (((0,), (0,)), ((), ())),
            preferred_element_type=jnp.float32,
        )

    def slot_copy(ref, sems, k, s, step, src):
        spot_of = (0 if s == 1 else reach[k][1]) + step
        return pltpu.make_async_remote_copy(
            src_ref=src,
            dst_ref=ref(spot_of),
            send_sem=sems[0].at[k, spot_of],
            recv_sem=sems[1].at[k, spot_of],
            device_id={"dp": target[s]},
            device_id_type=pl.DeviceIdType.MESH,
        )

    def sum_copy(k, s, step, first=False):
        before_it = (0 if s == 1 else reach[k][1]) + step - 1
        src = first_ref.at[k, (1 - s) // 2] if first else acc_ref.at[k, before_it]
        return slot_copy(lambda i: acc_ref.at[k, i], (rs_send, rs_recv), k, s, step, src)

    def gather_copy(k, s, step, owner):
        block = gath_ref.at[owner, k]
        return slot_copy(lambda i: block, (ag_send, ag_recv), k, s, step, block)

    def arrived(k, s, step):
        sum_copy(k, s, step, True).wait_recv()
        return acc_ref[k, (0 if s == 1 else reach[k][1]) + step].astype(jnp.float32)

    def sum_open(k, s):
        first_ref[k, (1 - s) // 2] = term(here + s * reach[k][s], k).astype(jnp.bfloat16)

    def pass_on(k, s, step):
        own = term(here + s * (reach[k][s] - step), k)
        total = (arrived(k, s, step - 1) + own).astype(jnp.bfloat16)
        acc_ref[k, (0 if s == 1 else reach[k][1]) + step - 1] = total
        sum_copy(k, s, step).start()

    def settle(k):
        total = term(here, k)
        for s in sides[k]:
            total = total + arrived(k, s, reach[k][s] - 1)
        grad_ref[k] = total.astype(jnp.bfloat16)

    def relay(k, s, step):
        owner = at_spot(here - s * (1 + step), n)
        gather_copy(k, s, step, owner).wait_recv()
        gather_copy(k, s, step + 1, owner).start()

    def arrive(k, s):
        last = reach[k][s] - 1
        gather_copy(k, s, last, at_spot(here - s * (1 + last), n)).wait_recv()

    row = lax.broadcasted_iota(jnp.int32, (width, width), 0)
    col = lax.broadcasted_iota(jnp.int32, (width, width), 1)
    identity = jnp.where(row == col, 1.0, 0.0).astype(jnp.float32)
    dot = functools.partial(jnp.dot, preferred_element_type=jnp.float32)

    def newton(k):
        g = grad_ref[k]
        gram = lax.dot_general(g, g, (((1,), (1,)), ((), ())), preferred_element_type=jnp.float32)
        renewed = decay_rate * old_ref[k] + (1.0 - decay_rate) * (gram / width)
        stats_ref[k] = renewed
        norm = jnp.sqrt(jnp.sum(renewed * renewed, keepdims=True) + 1e-06)
        mat_ref[k] = renewed / norm
        yield
        for step in range(ITERS):
            low = ((5.0 * identity - mat_ref[k]) / 4.0).astype(jnp.bfloat16)
            if step == 0:
                iter_ref[k] = low
            elif step + 1 < ITERS:
                iter_ref[k] = dot(iter_ref[k], low).astype(jnp.bfloat16)
            if step + 1 < ITERS:
                square = dot(low, low).astype(jnp.bfloat16)
                yield
                fourth = dot(square, square).astype(jnp.bfloat16)
                yield
                mat_ref[k] = dot(fourth, mat_ref[k].astype(jnp.bfloat16))
                yield
        root = dot(iter_ref[k], low) * norm ** (-0.25)
        yield
        gath_ref[me, k] = dot(root.astype(jnp.bfloat16), grad_ref[k]).astype(jnp.bfloat16)
        for s in sides[k]:
            gather_copy(k, s, 0, me).start()

    def advance(works, count=None):
        while works and count != 0:
            works = [work for work in works if next(work, True) is None]
            count = None if count is None else count - 1
        return works

    def loop(start, stop, body):
        lax.fori_loop(start, stop, lambda i, _: (body(i), 0)[1], 0)

    for cut in cuts:
        cut.wait()
    def arms(group, ends=sides):
        return [(k, s) for k in group for s in ends[k]]

    for k, s in arms(early):
        sum_open(k, s)
        if (k, s) == (early[0], sides[early[0]][0]):
            pl.semaphore_wait(barrier, 2)
        sum_copy(k, s, 0, True).start()
    ahead = [
        pltpu.make_async_copy(weight_hbm, weight_ref, ahead_sem.at[0]),
        pltpu.make_async_copy(next_hbm, next_ref, ahead_sem.at[1]),
    ]
    for load in ahead:
        load.start()
    for k, s in arms(late):
        sum_open(k, s)
    for k, s in arms(early):
        pass_on(k, s, 1)
    for k, s in arms(late):
        sum_copy(k, s, 0, True).start()

    def sum_step(i):
        for k, s in arms(early):
            pass_on(k, s, i)
        for k, s in arms(late):
            pass_on(k, s, i - 1)

    loop(2, least, sum_step)
    for k, s in arms(early, far):
        pass_on(k, s, least)
    for k, s in arms(late):
        pass_on(k, s, least - 1)
    for k in early:
        settle(k)
    load_old.wait()
    works = advance([newton(k) for k in early], HEAD)
    for k, s in arms(late, far):
        pass_on(k, s, least)
    advance(works)
    for k in late[:1]:
        settle(k)
    for k, s in arms(early):
        relay(k, s, 0)
    works = advance([newton(k) for k in late[:1]], TAIL)
    for k in late[1:]:
        settle(k)
    advance(works + [newton(k) for k in late[1:]])

    def gather_step(i):
        for k, s in arms(early):
            relay(k, s, i)
        for k, s in arms(late):
            relay(k, s, i - 1)

    loop(1, least - 1, gather_step)
    for k, s in arms(early, far):
        relay(k, s, least - 1)
    for k, s in arms(late):
        relay(k, s, least - 2)
    for k, s in arms(late, far):
        relay(k, s, least - 1)
    for k, s in arms(early + late):
        arrive(k, s)
    for load in ahead:
        load.wait()

    for k, s in arms(early + late):
        for step in (0, reach[k][s]):
            if step:
                loop(1, step, lambda i, k=k, s=s: sum_copy(k, s, i).wait_send())
                loop(1, step, lambda i, k=k, s=s: gather_copy(k, s, i, me).wait_send())
            else:
                sum_copy(k, s, 0, True).wait_send()
                gather_copy(k, s, 0, me).wait_send()


def refresh(n, row_of, col_of, activations, cotangent, old, weight, next_acts):
    slots, width, _ = old.shape
    tokens = activations.shape[0]
    vmem = pl.BlockSpec(memory_space=pltpu.VMEM)
    smem = pl.BlockSpec(memory_space=pltpu.SMEM)
    hbm = pl.BlockSpec(memory_space=pltpu.HBM)
    dma = pltpu.SemaphoreType.DMA
    low = jnp.bfloat16
    return pl.pallas_call(
        functools.partial(refresh_kernel, n, slots, width),
        out_shape=(
            jax.ShapeDtypeStruct((slots, width, width), jnp.float32),
            jax.ShapeDtypeStruct((n, slots, width, width), low),
            jax.ShapeDtypeStruct(weight.shape, weight.dtype),
            jax.ShapeDtypeStruct(next_acts.shape, next_acts.dtype),
        ),
        in_specs=[smem, smem, hbm, hbm, hbm, hbm, hbm],
        out_specs=(vmem, vmem, vmem, vmem),
        scratch_shapes=[
            pltpu.VMEM((activations.shape[1] // width, tokens, width), low),
            pltpu.VMEM((cotangent.shape[1] // width, tokens, width), low),
            pltpu.VMEM((slots, width, width), jnp.float32),
            pltpu.VMEM((slots, 2, width, width), low),
            pltpu.VMEM((slots, n - 1, width, width), low),
            pltpu.VMEM((slots, width, width), low),
            pltpu.VMEM((slots, width, width), jnp.float32),
            pltpu.VMEM((slots, width, width), low),
            dma((slots, n - 1)),
            dma((slots, n - 1)),
            dma((slots, n - 1)),
            dma((slots, n - 1)),
            dma((activations.shape[1] // width,)),
            dma((cotangent.shape[1] // width,)),
            dma,
            dma((2,)),
        ],
        compiler_params=pltpu.CompilerParams(
            vmem_limit_bytes=REFRESH_BYTES if n * slots <= 32 else VMEM_BYTES,
            collective_id=0,
            has_side_effects=True,
        ),
        cost_estimate=pl.CostEstimate(
            flops=2 * slots * 31 * width**3, bytes_accessed=100_000_000, transcendentals=0
        ),
        name="refresh",
    )(
        row_of, col_of,
        *(pltpu.with_memory_space_constraint(x, pltpu.HBM) for x in (activations, cotangent, old, weight, next_acts)),
    )


def total_kernel(n, part_ref, out_ref, near_ref, pair_ref, far_ref, near_send, near_recv, far_send, far_recv):
    me = lax.axis_index("feat")
    core = lax.rem(me, 2)
    here = me // 2
    chips = n // 2
    partner = here * 2 + 1 - core
    barrier = pltpu.get_barrier_semaphore()
    peers = [lax.rem(here + d, chips) * 2 + core for d in range(1, chips)]
    for peer in peers + [partner]:
        pl.semaphore_signal(
            barrier, inc=1, device_id={"feat": peer}, device_id_type=pl.DeviceIdType.MESH
        )
    pl.semaphore_wait(barrier, chips)

    def near_copy(d):
        place = lax.rem(here + d, chips) * 2 + 1 - core
        return pltpu.make_async_remote_copy(
            src_ref=part_ref.at[place],
            dst_ref=near_ref.at[d],
            send_sem=near_send.at[d],
            recv_sem=near_recv.at[d],
            device_id={"feat": partner},
            device_id_type=pl.DeviceIdType.MESH,
        )

    def far_copy(d):
        return pltpu.make_async_remote_copy(
            src_ref=pair_ref.at[d - 1],
            dst_ref=far_ref.at[d - 1],
            send_sem=far_send.at[d - 1],
            recv_sem=far_recv.at[d - 1],
            device_id={"feat": peers[d - 1]},
            device_id_type=pl.DeviceIdType.MESH,
        )

    def pair_sum(d):
        place = lax.rem(here + d, chips) * 2 + core
        own = part_ref[place].astype(jnp.float32)
        return own + near_ref[d].astype(jnp.float32)

    turns = list(range(1, chips)) + [0]
    for d in turns:
        near_copy(d).start()
    for d in turns[:-1]:
        near_copy(d).wait_recv()
        pair_ref[d - 1] = pair_sum(d).astype(pair_ref.dtype)
        far_copy(d).start()
    near_copy(0).wait_recv()
    total = pair_sum(0)
    for d in turns[:-1]:
        far_copy(d).wait_recv()
        total = total + far_ref[d - 1].astype(jnp.float32)
    out_ref[...] = total.astype(out_ref.dtype)
    for d in turns:
        near_copy(d).wait_send()
    for d in turns[:-1]:
        far_copy(d).wait_send()


def total_over_feat(n, parts):
    _, tokens, cols = parts.shape
    vmem = pl.BlockSpec(memory_space=pltpu.VMEM)
    dma = pltpu.SemaphoreType.DMA
    chips = n // 2
    return pl.pallas_call(
        functools.partial(total_kernel, n),
        out_shape=jax.ShapeDtypeStruct((tokens, cols), parts.dtype),
        in_specs=[vmem],
        out_specs=vmem,
        scratch_shapes=[
            pltpu.VMEM((chips, tokens, cols), parts.dtype),
            pltpu.VMEM((chips - 1, tokens, cols), parts.dtype),
            pltpu.VMEM((chips - 1, tokens, cols), parts.dtype),
            dma((chips,)),
            dma((chips,)),
            dma((chips - 1,)),
            dma((chips - 1,)),
        ],
        compiler_params=pltpu.CompilerParams(
            vmem_limit_bytes=TOTAL_BYTES, collective_id=1, has_side_effects=True
        ),
        name="total_over_feat",
    )(parts)


def apply_kernel(
    width, col_blocks, splits, place_ref, weight_ref, acts_ref, gath_ref, stats_ref,
    new_hbm, part_ref, stats_hbm, fresh_ref, low_ref, new_sem, stats_sem,
):
    row_blocks = weight_ref.shape[0] // width
    share = weight_ref.shape[1] // splits
    keep = pltpu.make_async_copy(stats_ref, stats_hbm, stats_sem)
    keep.start()
    writes = []

    def renew(c, r):
        rows, cols = slice(r * width, (r + 1) * width), slice(c * width, (c + 1) * width)
        update = gath_ref[place_ref[r * col_blocks + c]]
        fresh = weight_ref[rows, cols] - step_rate * update.astype(jnp.float32)
        fresh_ref[rows, cols] = fresh
        low_ref[c, rows, :] = fresh.astype(jnp.bfloat16)
        copy = pltpu.make_async_copy(
            fresh_ref.at[rows, cols], new_hbm.at[rows, cols], new_sem.at[c, r]
        )
        copy.start()
        writes.append(copy)

    def write(c):
        return

        cols = slice(c * width, (c + 1) * width)
        copy = pltpu.make_async_copy(fresh_ref.at[:, cols], new_hbm.at[:, cols], new_sem.at[c])
        copy.start()
        writes.append(copy)

    for r in range(row_blocks):
        renew(0, r)
    write(0)
    for c in range(col_blocks):
        part = jnp.zeros((acts_ref.shape[0], width), jnp.float32)
        for r in range(row_blocks):
            rows = slice(r * width, (r + 1) * width)
            part = part + jnp.dot(
                acts_ref[:, rows], low_ref[c, rows, :], preferred_element_type=jnp.float32
            )
            if c + 1 < col_blocks:
                renew(c + 1, r)
        if c + 1 < col_blocks:
            write(c + 1)
        part = part.astype(part_ref.dtype)
        if share >= width:
            spot_in = (c * width) % share
            part_ref[(c * width) // share, :, spot_in : spot_in + width] = part
        else:
            for f in range(width // share):
                part_ref[(c * width) // share + f] = part[:, f * share : (f + 1) * share]
    for copy in writes:
        copy.wait()
    keep.wait()


def apply_update(place, weight, acts, gathered, stats, splits):
    width = gathered.shape[-1]
    rows, cols = weight.shape
    tokens = acts.shape[0]
    share = cols // splits
    vmem = pl.BlockSpec(memory_space=pltpu.VMEM)
    hbm = pl.BlockSpec(memory_space=pltpu.HBM)
    return pl.pallas_call(
        functools.partial(apply_kernel, width, cols // width, splits),
        out_shape=(
            jax.ShapeDtypeStruct((rows, cols), jnp.float32),
            jax.ShapeDtypeStruct((splits, tokens, share), jnp.bfloat16),
            jax.ShapeDtypeStruct(stats.shape, stats.dtype),
        ),
        in_specs=[pl.BlockSpec(memory_space=pltpu.SMEM), vmem, vmem, vmem, vmem],
        out_specs=(hbm, vmem, hbm),
        scratch_shapes=[
            pltpu.VMEM((rows, cols), jnp.float32),
            pltpu.VMEM((cols // width, rows, width), jnp.bfloat16),
            pltpu.SemaphoreType.DMA((cols // width, rows // width)),
            pltpu.SemaphoreType.DMA,
        ],
        compiler_params=pltpu.CompilerParams(
            vmem_limit_bytes=APPLY_BYTES if gathered.size <= 1 << 21 else VMEM_BYTES,
        ),
        cost_estimate=pl.CostEstimate(
            flops=2 * rows * cols * tokens,
            bytes_accessed=8 * rows * cols + 2 * gathered.size,
            transcendentals=0,
        ),
        name="apply_update",
    )(place, weight, acts, gathered, stats)


def body(n_dp, n_feat, activations, cotangent, weight, stats_old, owners, next_acts):
    width = stats_old.shape[-1]
    slots = stats_old.shape[2]
    rows_dev, columns = weight.shape
    row_blocks = rows_dev // width
    col_blocks = columns // width
    block_count = row_blocks * col_blocks
    feat_index = lax.axis_index("feat")
    data_index = lax.axis_index("dp")
    own_list = lax.dynamic_slice_in_dim(owners, feat_index * row_blocks, row_blocks, 0).reshape(
        block_count
    )
    ids = jnp.arange(block_count, dtype=jnp.int32)
    slot_of = jnp.sum(
        ((own_list[:, None] == own_list[None, :]) & (ids[None, :] < ids[:, None])).astype(jnp.int32),
        axis=1,
    )
    place = own_list * slots + slot_of
    held = place[None, :] == jnp.arange(n_dp * slots, dtype=jnp.int32)[:, None]
    order = jnp.sum(jnp.where(held, ids[None, :], 0), axis=1)
    stats, gathered, weight, next_acts = refresh(
        n_dp, order // col_blocks, order % col_blocks, activations, cotangent, stats_old[0, 0],
        weight, next_acts,
    )
    if n_dp * slots != block_count:
        mine = (own_list == data_index)[None, :] & (slot_of[None, :] == jnp.arange(slots)[:, None])
        stats = jnp.where(jnp.any(mine, axis=1)[:, None, None], stats, 0.0)
    gathered = gathered.reshape(n_dp * slots, width, width)
    direct = columns % (128 * n_feat) == 0 and n_feat % 2 == 0 and n_feat > 2
    weight_new, parts, stats = apply_update(
        place, weight, next_acts, gathered, stats, n_feat if direct else 1
    )
    if direct:
        next_out = total_over_feat(n_feat, parts)
    else:
        next_out = lax.psum_scatter(parts[0], "feat", scatter_dimension=1, tiled=True)
    return (weight_new, stats[None, None], next_out)


def solution(mesh):
    placed = (
        P("dp", "feat"),
        P("dp", None),
        P("feat", None),
        P("feat", "dp", None, None, None),
        P(),
        P("dp", "feat"),
    )
    return jax.shard_map(
        functools.partial(body, mesh.shape["dp"], mesh.shape["feat"]),
        mesh=mesh,
        in_specs=placed,
        out_specs=(P("feat", None), P("feat", "dp", None, None, None), P("dp", "feat")),
        check_vma=False,
    )
```
